256 devices in a mesh: ctx: 16 (over z, core), rep: 4 (over y), tp: 4 (over x).
Axes of the slice: x: 4, y: 4, z: 8, core: 2. Of those that a mesh axis runs over, the one named last changes fastest.
Arguments:
- prompt_x: bfloat16 [16384, 16384], P(('ctx', 'rep'), 'tp'), may hold values from -6 to 6
- prompt_z: bfloat16 [16384, 16384], P(('ctx', 'rep'), 'tp'), may hold values from -6 to 6
- prompt_b: bfloat16 [16384, 1024], P(('ctx', 'rep'), 'tp'), may hold values from -1.25 to 1.25
- prompt_c: bfloat16 [16384, 1024], P(('ctx', 'rep'), 'tp'), may hold values from -1.25 to 1.25
- prompt_dt: float32 [16384, 256], P(('ctx', 'rep'), 'tp'), may hold values from 0.2 to 1.2
- rate_log: float32 [256], P('tp'), may hold values from -30 to -2
- skip_scale: float32 [256], P('tp'), may hold values from 0.5 to 1.5
- norm_gain: float32 [16384], P('tp'), may hold values from 0.5 to 1.5
- prefix_key_rows: bfloat16 [16384, 1024], P(('ctx', 'rep'), 'tp'), may hold values from -6 to 6
- prefix_value_rows: bfloat16 [16384, 1024], P(('ctx', 'rep'), 'tp'), may hold values from -6 to 6
- fork_counts: int32 [64], P(('ctx', 'rep')), may hold values from 0 to 2, as said below
- fork_x: bfloat16 [128, 4, 16384], P(('ctx', 'rep'), None, 'tp'), may hold values from -6 to 6
- fork_z: bfloat16 [128, 4, 16384], P(('ctx', 'rep'), None, 'tp'), may hold values from -6 to 6
- fork_b: bfloat16 [128, 4, 1024], P(('ctx', 'rep'), None, 'tp'), may hold values from -1.25 to 1.25
- fork_c: bfloat16 [128, 4, 1024], P(('ctx', 'rep'), None, 'tp'), may hold values from -1.25 to 1.25
- fork_dt: float32 [128, 4, 256], P(('ctx', 'rep'), None, 'tp'), may hold values from 0.2 to 1.2
- fork_queries: bfloat16 [128, 4, 8192], P(('ctx', 'rep'), None, 'tp'), may hold values from -16 to 16
- fork_keys: bfloat16 [128, 4, 1024], P(('ctx', 'rep'), None, 'tp'), may hold values from -16 to 16
- branch_value_rows: bfloat16 [128, 4, 1024], P(('ctx', 'rep'), None, 'tp'), may hold values from -6 to 6
Outputs:
- prompt_out: bfloat16 [16384, 16384], P(('ctx', 'rep'), 'tp')
- fork_mamba: bfloat16 [128, 4, 16384], P(('ctx', 'rep'), None, 'tp')
- fork_attn: bfloat16 [128, 4, 8192], P(('ctx', 'rep'), None, 'tp')
The draws below stay inside these ranges and needn't reach their ends.
Inputs may be any that keep to these rules, and one draw needn't show every extreme that they name: `fork_counts`: after each segment at most 2 forks branch off; in every draw some segment has exactly 2.
All inputs are finite; a program needn't handle non-finite values.
Results may differ from the reference program's by a relative error of at most 0.00155.
Values may be sent and summed in bfloat16 or wider, within the bound.
No kernel may reach another device: no remote copies, remote signals or barrier semaphores. Data moves between devices by JAX's collectives and lax.ppermute only.
A program may use at most 384 MiB of HBM per device.

```python
import math
import jax
import jax.numpy as jnp
from jax import lax

H = 256
P_SIZE = 64
N = 128
G = 8
QUERY_HEADS = 64
KEY_VALUE_HEADS = 8
HEAD_DIMENSION = 128
TOK_DEV = 256
SEGMENT_SLOTS = 2
FORK_STEPS = 4
SEGMENTS = 64
PROMPT_TOKENS = 16384
TOTAL_SLOTS = 128
N_CTX = 16
N_REP = 4


def draw_rate_log(key, part):
    fast_end = jnp.log(0.08)
    slow_end = jnp.log(0.5 / PROMPT_TOKENS)
    spread = jax.random.uniform(jax.random.fold_in(key, 5), (H,), jnp.float32)
    return (slow_end + spread * (fast_end - slow_end)).astype(jnp.float32)


def draw_fork_counts(key, part):
    counts_drawn = jax.random.randint(jax.random.fold_in(key, 7), (SEGMENTS,), 0, SEGMENT_SLOTS + 1)
    fullest = jax.random.randint(jax.random.fold_in(key, 8), (), 0, SEGMENTS)
    return counts_drawn.at[fullest].set(SEGMENT_SLOTS).astype(jnp.int32)


def attention_pair(key):
    query_matrix = jax.random.normal(jax.random.fold_in(key, 21), (TOTAL_SLOTS, FORK_STEPS, QUERY_HEADS * HEAD_DIMENSION), jnp.float32)
    query_matrix = jnp.clip(query_matrix, -16.0, 16.0)
    leading_slots = query_matrix.reshape(TOTAL_SLOTS, FORK_STEPS, KEY_VALUE_HEADS, QUERY_HEADS // KEY_VALUE_HEADS, HEAD_DIMENSION)[:, :, :, 0, :]
    random_portion = jax.random.normal(jax.random.fold_in(key, 23), (TOTAL_SLOTS, FORK_STEPS, KEY_VALUE_HEADS, HEAD_DIMENSION), jnp.float32)
    self_key_rows = jnp.clip(0.6 * leading_slots + 0.8 * random_portion, -16.0, 16.0).reshape(TOTAL_SLOTS, FORK_STEPS, KEY_VALUE_HEADS * HEAD_DIMENSION)
    return (query_matrix, self_key_rows)


def draw_fork_queries(key, part):
    return attention_pair(key)[0].astype(jnp.bfloat16)


def draw_fork_keys(key, part):
    return attention_pair(key)[1].astype(jnp.bfloat16)


def steps_of(stream_key, dims, shards, least, largest):
    def one(dim, shards_of):
        steps = jax.random.uniform(jax.random.fold_in(jax.random.fold_in(stream_key, 6), dim), (shards_of,), jnp.float32, least / len(shards), largest / len(shards))
        return jnp.repeat(jnp.exp(steps), dims[dim] // shards_of).reshape((-1,) + (1,) * (len(dims) - dim - 1))

    factor_of = one(*shards[0])
    for cut in shards[1:]:
        factor_of = factor_of * one(*cut)
    return factor_of


def normal_values(stream_key, shape, deviation, bound, cuts=(), dtype=jnp.bfloat16):
    entries = jax.random.normal(stream_key, shape, jnp.float32) * deviation
    if len(cuts) > 0:
        entries = steps_of(stream_key, shape, cuts, -0.22, 0.18) * entries
    return jnp.clip(entries, min=-bound, max=bound).astype(dtype)


def setup_inputs(seed: int = 0) -> dict:
    seeds = jax.random.split(jax.random.key(seed), 20)
    return {
        "prompt_x": normal_values(seeds[0], (PROMPT_TOKENS, H * P_SIZE), 1.0, 6.0, ((0, 64), (1, 4))),
        "prompt_z": normal_values(seeds[1], (PROMPT_TOKENS, H * P_SIZE), 1.0, 6.0, ((0, 64), (1, 4))),
        "prompt_b": normal_values(seeds[2], (PROMPT_TOKENS, G * N), (N ** -0.5), 1.25, ((0, 64), (1, 4))),
        "prompt_c": normal_values(seeds[3], (PROMPT_TOKENS, G * N), (N ** -0.5), 1.25, ((0, 64), (1, 4))),
        "prompt_dt": jnp.clip(jnp.exp(math.log(1.2) - 1.7917595 * jax.random.uniform(seeds[4], (PROMPT_TOKENS, H), jnp.float32) ** steps_of(seeds[4], (PROMPT_TOKENS, H), ((0, 64), (1, 4)), -0.2, 0.2)), 0.2, 1.2),
        "rate_log": draw_rate_log(jax.random.fold_in(seeds[19], 71), 0),
        "skip_scale": jnp.clip(0.5 + 1.0 * jax.random.uniform(seeds[6], (H,), jnp.float32) ** steps_of(seeds[6], (H,), ((0, 4),), -0.2, 0.2), 0.5, 1.5),
        "norm_gain": jnp.clip(1.0 + 0.1 * jax.random.normal(seeds[7], (H * P_SIZE,), jnp.float32), 0.5, 1.5),
        "prefix_key_rows": normal_values(seeds[8], (PROMPT_TOKENS, KEY_VALUE_HEADS * HEAD_DIMENSION), 1.0, 6.0, ((0, 64), (1, 4))),
        "prefix_value_rows": normal_values(seeds[9], (PROMPT_TOKENS, KEY_VALUE_HEADS * HEAD_DIMENSION), 1.0, 6.0, ((0, 64), (1, 4))),
        "fork_counts": draw_fork_counts(jax.random.fold_in(seeds[19], 71), 0),
        "fork_x": normal_values(seeds[11], (TOTAL_SLOTS, FORK_STEPS, H * P_SIZE), 1.0, 6.0, ((0, 64), (2, 4))),
        "fork_z": normal_values(seeds[12], (TOTAL_SLOTS, FORK_STEPS, H * P_SIZE), 1.0, 6.0, ((0, 64), (2, 4))),
        "fork_b": normal_values(seeds[13], (TOTAL_SLOTS, FORK_STEPS, G * N), (N ** -0.5), 1.25, ((0, 64), (2, 4))),
        "fork_c": normal_values(seeds[14], (TOTAL_SLOTS, FORK_STEPS, G * N), (N ** -0.5), 1.25, ((0, 64), (2, 4))),
        "fork_dt": jnp.clip(jnp.exp(math.log(1.2) - 1.7917595 * jax.random.uniform(seeds[15], (TOTAL_SLOTS, FORK_STEPS, H), jnp.float32) ** steps_of(seeds[15], (TOTAL_SLOTS, FORK_STEPS, H), ((0, 64), (2, 4)), -0.2, 0.2)), 0.2, 1.2),
        "fork_queries": draw_fork_queries(jax.random.fold_in(seeds[19], 71), 0),
        "fork_keys": draw_fork_keys(jax.random.fold_in(seeds[19], 71), 0),
        "branch_value_rows": normal_values(seeds[18], (TOTAL_SLOTS, FORK_STEPS, KEY_VALUE_HEADS * HEAD_DIMENSION), 1.0, 6.0, ((0, 64), (2, 4))),
    }


HIGHEST = lax.Precision.HIGHEST
EPSILON = 1e-05

def expand_groups(values, head_count, state_depth):
    leading = values.shape[:-1]
    groups = values.shape[-1] // state_depth
    shaped = values.reshape(leading + (groups, state_depth))
    return jnp.repeat(shaped, head_count // groups, axis=len(leading)).astype(jnp.float32)

def ssd_block(state_now, block_x, block_b, block_c, block_dt, decay_rates, skip_scale):
    length, head_count = block_dt.shape
    head_width, state_depth = (state_now.shape[1], state_now.shape[2])
    groups = block_b.shape[1] // state_depth
    cumulated = jnp.cumsum(block_dt * decay_rates[None, :], axis=0)
    x_heads = block_x.reshape(length, head_count, head_width).astype(jnp.float32)
    inputs = x_heads * block_dt[:, :, None]
    pairing = jnp.einsum('tgn,sgn->gts', block_c.reshape(length, groups, state_depth), block_b.reshape(length, groups, state_depth), preferred_element_type=jnp.float32)
    pairing = jnp.repeat(pairing, head_count // groups, axis=0)
    log_gaps = cumulated.T[:, :, None] - cumulated.T[:, None, :]
    lower_mask = (jnp.arange(length)[:, None] >= jnp.arange(length)[None, :])[None]
    mixing = jnp.where(lower_mask, jnp.exp(jnp.where(lower_mask, log_gaps, 0.0)), 0.0) * pairing
    inside = jnp.einsum('hts,shp->thp', mixing, inputs, precision=HIGHEST)
    c_heads = expand_groups(block_c, head_count, state_depth)
    b_heads = expand_groups(block_b, head_count, state_depth)
    carried = jnp.einsum('thn,hpn->thp', c_heads, state_now, precision=HIGHEST) * jnp.exp(cumulated)[:, :, None]
    output = inside + carried + skip_scale[None, :, None] * x_heads
    remaining = jnp.exp(cumulated[-1][None, :] - cumulated)
    fresh_part = jnp.einsum('shp,shn->hpn', inputs * remaining[:, :, None], b_heads, precision=HIGHEST)
    new_state = jnp.exp(cumulated[-1])[:, None, None] * state_now + fresh_part
    return (new_state, output, c_heads)

def fork_update(fork_state, step_x, step_b, step_c, step_dt, decay_rates, skip_scale):
    slot_count, head_count = step_dt.shape
    head_width, state_depth = (fork_state.shape[2], fork_state.shape[3])
    x_heads = step_x.reshape(slot_count, head_count, head_width).astype(jnp.float32)
    b_heads = expand_groups(step_b, head_count, state_depth)
    c_heads = expand_groups(step_c, head_count, state_depth)
    decays = jnp.exp(step_dt * decay_rates[None, :])
    fork_state = decays[:, :, None, None] * fork_state + (x_heads * step_dt[:, :, None])[:, :, :, None] * b_heads[:, :, None, :]
    output = jnp.einsum('mhpn,mhn->mhp', fork_state, c_heads, precision=HIGHEST) + skip_scale[None, :, None] * x_heads
    return (fork_state, output)

def gate_terms(output, gate_in):
    return output * jax.nn.silu(gate_in.astype(jnp.float32).reshape(output.shape))

def normalize(gated, gain_table):
    mean_square = lax.optimization_barrier(jnp.mean(gated * gated, axis=(-2, -1)))
    return gated * lax.rsqrt(mean_square + EPSILON)[..., None, None] * gain_table

def reference(prompt_x, prompt_z, prompt_b, prompt_c, prompt_dt, rate_log, skip_scale, norm_gain, prefix_key_rows, prefix_value_rows, fork_counts, fork_x, fork_z, fork_b, fork_c, fork_dt, fork_queries, fork_keys, branch_value_rows):
    decay_rates = -jnp.exp(rate_log)
    segment_count = N_CTX * N_REP
    block_rows = min(128, TOK_DEV)
    gain_table = norm_gain.reshape(H, P_SIZE)
    query_group_width = QUERY_HEADS // KEY_VALUE_HEADS
    score_scale = HEAD_DIMENSION ** (-0.5)
    joined_keys = prefix_key_rows.reshape(PROMPT_TOKENS, KEY_VALUE_HEADS, HEAD_DIMENSION)
    joined_values = prefix_value_rows.reshape(PROMPT_TOKENS, KEY_VALUE_HEADS, HEAD_DIMENSION).astype(jnp.float32)
    positions = jnp.arange(PROMPT_TOKENS)
    causal_mask = (jnp.arange(FORK_STEPS)[:, None] >= jnp.arange(FORK_STEPS)[None, :])[None, None, :, None, :]

    def per_segment(values):
        return values.reshape((segment_count, values.shape[0] // segment_count) + values.shape[1:])

    def segment_step(state_now, inputs):
        seg_index, seg_x, seg_z, seg_b, seg_c, seg_dt, fork_count, slot_x, slot_z, slot_b, slot_c, slot_dt, slot_query_rows, slot_key_rows, slot_value_rows = inputs
        pieces = []
        for block_start in range(0, TOK_DEV, block_rows):
            block_end = block_start + block_rows
            state_now, output, c_heads = ssd_block(state_now, seg_x[block_start:block_end], seg_b[block_start:block_end], seg_c[block_start:block_end], seg_dt[block_start:block_end], decay_rates, skip_scale)
            pieces.append(output)
        prompt_gated = gate_terms(jnp.concatenate(pieces, axis=0), seg_z)
        prompt_rows = normalize(prompt_gated, gain_table).astype(jnp.bfloat16).reshape(TOK_DEV, H * P_SIZE)
        live_slots = (jnp.arange(SEGMENT_SLOTS) < fork_count).astype(jnp.float32)
        fork_state = jnp.broadcast_to(state_now, (SEGMENT_SLOTS,) + state_now.shape)
        gated_steps = []
        for step_index in range(FORK_STEPS):
            fork_state, output = fork_update(fork_state, slot_x[:, step_index], slot_b[:, step_index], slot_c[:, step_index], slot_dt[:, step_index], decay_rates, skip_scale)
            gated_steps.append(gate_terms(output, slot_z[:, step_index]))
        fork_gated = jnp.stack(gated_steps, axis=1)
        mamba_rows = (normalize(fork_gated, gain_table) * live_slots[:, None, None, None]).astype(jnp.bfloat16).reshape(SEGMENT_SLOTS, FORK_STEPS, H * P_SIZE)
        query_matrix = slot_query_rows.reshape(SEGMENT_SLOTS, FORK_STEPS, KEY_VALUE_HEADS, query_group_width, HEAD_DIMENSION)
        key_limit = (seg_index + 1) * TOK_DEV
        prompt_scores = jnp.einsum('msgqd,tgd->gmsqt', query_matrix, joined_keys, preferred_element_type=jnp.float32) * score_scale
        prompt_scores = jnp.where(positions < key_limit, prompt_scores, -jnp.inf)
        self_key_rows = slot_key_rows.reshape(SEGMENT_SLOTS, FORK_STEPS, KEY_VALUE_HEADS, HEAD_DIMENSION)
        self_value_rows = slot_value_rows.reshape(SEGMENT_SLOTS, FORK_STEPS, KEY_VALUE_HEADS, HEAD_DIMENSION).astype(jnp.float32)
        own_scores = jnp.einsum('msgqd,mtgd->gmsqt', query_matrix, self_key_rows, preferred_element_type=jnp.float32) * score_scale
        own_scores = jnp.where(causal_mask, own_scores, -jnp.inf)
        peak_score = jnp.maximum(lax.optimization_barrier(jnp.max(prompt_scores, axis=-1)), lax.optimization_barrier(jnp.max(own_scores, axis=-1)))
        prompt_weights = jnp.exp(prompt_scores - peak_score[..., None])
        own_weights = jnp.exp(own_scores - peak_score[..., None])
        weight_sum = lax.optimization_barrier(jnp.sum(prompt_weights, axis=-1)) + lax.optimization_barrier(jnp.sum(own_weights, axis=-1))
        weighted = jnp.einsum('gmsqt,tgd->gmsqd', prompt_weights, joined_values, precision=HIGHEST) + jnp.einsum('gmsqt,mtgd->gmsqd', own_weights, self_value_rows, precision=HIGHEST)
        attended = weighted / weight_sum[..., None]
        attn_rows = (jnp.transpose(attended, (1, 2, 0, 3, 4)) * live_slots[:, None, None, None, None]).astype(jnp.bfloat16).reshape(SEGMENT_SLOTS, FORK_STEPS, QUERY_HEADS * HEAD_DIMENSION)
        return (state_now, (prompt_rows, mamba_rows, attn_rows))
    sequence = (jnp.arange(segment_count), per_segment(prompt_x), per_segment(prompt_z), per_segment(prompt_b), per_segment(prompt_c), per_segment(prompt_dt), fork_counts, per_segment(fork_x), per_segment(fork_z), per_segment(fork_b), per_segment(fork_c), per_segment(fork_dt), per_segment(fork_queries), per_segment(fork_keys), per_segment(branch_value_rows))
    start_state = jnp.zeros((H, P_SIZE, N), jnp.float32)
    final_state, results = lax.scan(segment_step, start_state, sequence)
    prompt_rows, mamba_rows, attn_rows = results
    return (prompt_rows.reshape(PROMPT_TOKENS, H * P_SIZE), mamba_rows.reshape(TOTAL_SLOTS, FORK_STEPS, H * P_SIZE), attn_rows.reshape(TOTAL_SLOTS, FORK_STEPS, QUERY_HEADS * HEAD_DIMENSION))
```

```python
import functools

import jax
import jax.numpy as jnp
from jax import lax
from jax.experimental import pallas as pl
from jax.experimental.pallas import tpu as pltpu
from jax.sharding import Mesh
from jax.sharding import PartitionSpec as P

P_SIZE = 64
N = 128
HEAD_DIMENSION = 128
CTX_REP = ("ctx_0", "ctx_1", "rep")
EPSILON = 1e-05
FLOOR_SCORE = -1e30
ROWS = 256
FORKS = 8
EXT = ROWS + FORKS
HEADS = 64
WIDTH = HEADS * P_SIZE
SHARD = WIDTH // 4
SHARD_HEADS = HEADS // 4
HALF = SHARD // 2
META = N + 8
TOP_CODE = 32760.0
F32 = jnp.float32
BF16 = jnp.bfloat16


def mm(a, b):
    return jnp.dot(a, b, preferred_element_type=F32)


def mm_nt(a, b):
    return lax.dot_general(a, b, (((1,), (1,)), ((), ())), preferred_element_type=F32)


def mm_tn(a, b):
    return lax.dot_general(a, b, (((0,), (0,)), ((), ())), preferred_element_type=F32)


def split2(v):
    hi = v.astype(BF16)
    return hi, (v - hi.astype(F32)).astype(BF16)


def split3(v):
    hi = v.astype(BF16)
    rest = v - hi.astype(F32)
    mid = rest.astype(BF16)
    return hi, mid, (rest - mid.astype(F32)).astype(BF16)


def iota(shape, axis):
    return lax.broadcasted_iota(jnp.int32, shape, axis)


def expand(values, shard):
    head = iota((HEADS, SHARD), 0)
    pick = (head == shard * SHARD_HEADS + iota((HEADS, SHARD), 1) // P_SIZE).astype(BF16)
    hi, mid, lo = split3(values)
    return mm(hi, pick) + mm(mid, pick) + mm(lo, pick)


def running_sum(a):
    rows = a.shape[0]
    tri = (iota((rows, rows), 0) >= iota((rows, rows), 1)).astype(BF16)
    hi, mid, lo = split3(a)
    return mm(tri, hi) + mm(tri, mid) + mm(tri, lo)


def encode(state, log_decay):
    width = state.shape[1]
    peak = jnp.max(jnp.abs(state), axis=0, keepdims=True)
    level = jnp.floor(jnp.log2(jnp.maximum(peak, 1e-30)) * 256.0) + 2.0
    codes = jnp.floor(state * (jnp.exp2(level * (-1.0 / 256.0)) * TOP_CODE) + 0.5)
    high = jnp.floor(log_decay * 16.0 + 0.5)
    low = jnp.floor((log_decay - high * (1.0 / 16.0)) * (16.0 * 32768.0) + 0.5)
    row = iota((8, width), 0)
    meta = jnp.where(row == 0, level, jnp.where(row == 1, high, jnp.where(row == 2, low, 0.0)))
    return jnp.concatenate([codes, meta], axis=0).astype(jnp.int32).astype(jnp.int16)


def decode(coded):
    v = coded.astype(jnp.int32).astype(F32)
    scale = jnp.exp2(v[N : N + 1] * (1.0 / 256.0)) * (1.0 / TOP_CODE)
    log_decay = v[N + 1 : N + 2] * (1.0 / 16.0) + v[N + 2 : N + 3] * (1.0 / (16.0 * 32768.0))
    return v[:N] * scale, log_decay


def with_log(state, log_decay):
    return jnp.concatenate([state, jnp.broadcast_to(log_decay, (8, state.shape[1]))], axis=0)


def call(kernel, pos, arrays, in_specs, outs, out_specs, grid=(1,), scratch=(), flops=10**8, alias=None, name=None):
    return pl.pallas_call(
        kernel,
        out_shape=outs,
        grid_spec=pltpu.PrefetchScalarGridSpec(
            num_scalar_prefetch=1,
            grid=grid,
            in_specs=in_specs,
            out_specs=out_specs,
            scratch_shapes=list(scratch),
        ),
        input_output_aliases=alias or {},
        compiler_params=pltpu.CompilerParams(
            dimension_semantics=("arbitrary",) * len(grid), vmem_limit_bytes=40 * 2**20
        ),
        cost_estimate=pl.CostEstimate(flops=flops, bytes_accessed=4 * 2**20, transcendentals=0),
        name=name,
    )(pos, *arrays)


def whole(shape):
    return pl.BlockSpec(shape, lambda i, pos: (0,) * len(shape))


def struct(shape, dtype=F32):
    return jax.ShapeDtypeStruct(shape, dtype)


def state_kernel(k, pos, dt_ref, rate_ref, x_ref, b_ref, out_ref):
    shard = lax.rem(pos[0] + k, 4)
    dt = dt_ref[...]
    cum = running_sum(dt * -jnp.exp(rate_ref[...]))
    scaled = x_ref[...].astype(F32) * expand(dt * jnp.exp(-cum), shard)
    hi, lo = split2(scaled)
    b = b_ref[...]
    last = expand(jnp.broadcast_to(cum[ROWS - 1 :], (8, HEADS)), shard)[:1]
    state = (mm_tn(b, hi) + mm_tn(b, lo)) * jnp.exp(last)
    out_ref[...] = encode(state, last)


def row_kernel(pos, *refs):
    parts, out_ref, buf = refs[:4], refs[4], refs[5]
    for k in range(4):
        buf[lax.rem(pos[0] + 4 - k, 4)] = parts[k][...]
    state, log_all = decode(buf[0])
    for y in range(1, 4):
        new, log_new = decode(buf[y])
        state = new + jnp.exp(log_new) * state
        log_all = log_all + log_new
    out_ref[...] = with_log(state, log_all)


def join(early, early_log, late, late_log):
    return late + jnp.exp(late_log) * early, early_log + late_log


def plane_kernel(pos, own_ref, other_ref, total_ref, coded_ref):
    own, other = own_ref[...], other_ref[...]
    first = pos[1] == 0
    early, late = jnp.where(first, own, other), jnp.where(first, other, own)
    state, log_all = join(early[:N], early[N : N + 1], late[:N], late[N : N + 1])
    total_ref[...] = with_log(state, log_all)
    coded_ref[...] = encode(state, log_all)


def scan_kernel(bit, last, pos, *refs):
    first = bit == 0
    if first:
        total_ref, got_ref, *outs = refs
    else:
        total_ref, before_ref, got_ref, *outs = refs
    got, got_log = decode(got_ref[...])
    later = (lax.rem(pos[2] // (1 << bit), 2) == 1).astype(F32)
    if first:
        before = got * later
        before_log = got_log * later
    else:
        before, before_log = before_ref[:N], before_ref[N : N + 1]
        before = before + jnp.exp(before_log) * (got * later)
        before_log = before_log + got_log * later
    outs[0][...] = with_log(before, before_log)
    if last:
        return
    total, total_log = total_ref[:N], total_ref[N : N + 1]
    joined = jnp.where(later > 0.0, total + jnp.exp(total_log) * got, got + jnp.exp(got_log) * total)
    log_all = total_log + got_log
    outs[1][...] = with_log(joined, log_all)
    outs[2][...] = encode(joined, log_all)


def return_kernel(pos, *refs):
    parts, own_ref, other_ref, row_ref, outs, buf, prefix = refs[:4], refs[4], refs[5], refs[6], refs[7:11], refs[11], refs[12]
    for k in range(4):
        buf[lax.rem(pos[0] + 4 - k, 4)] = parts[k][...]
    own, other = own_ref[:N], other_ref[:N]
    low = pos[1] == 0
    state = jnp.concatenate([jnp.where(low, own, other), jnp.where(low, other, own)], axis=1)
    after = row_ref[:N] + jnp.exp(row_ref[N : N + 1]) * state
    state = jnp.where(low, state, after)
    prefix[0] = state
    for y in range(3):
        new, log_new = decode(buf[y])
        state = new + jnp.exp(log_new) * state
        prefix[y + 1] = state
    zero = jnp.zeros((1, SHARD), F32)
    for k in (2, 1, 3, 0):
        outs[k][...] = encode(prefix[lax.rem(pos[0] + k, 4)], zero)


def local_kernel(pos, dt_ref, rate_ref, skip_ref, x_ref, z_ref, b_ref, c_ref, fdt_ref, fx_ref, fz_ref, fb_ref, fc_ref, g_ref, f_ref):
    shard = pl.program_id(0)
    rates = -jnp.exp(rate_ref[...])
    dt = dt_ref[...]
    cum = running_sum(dt * rates)
    last = cum[ROWS - 1 :]
    fdt = jnp.concatenate([fdt_ref[0], fdt_ref[1]], axis=0)
    step = iota((FORKS, FORKS), 0)
    prior = iota((FORKS, FORKS), 1)
    chain = (step >= prior) & (step // 4 == prior // 4)
    fa = fdt * rates
    forms = []
    for slot in range(2):
        total = jnp.zeros((1, HEADS), F32)
        for s in range(4):
            total = total + fa[slot * 4 + s : slot * 4 + s + 1]
            forms.append(total)
    fcum = jnp.concatenate(forms, axis=0) + last
    all_cum = jnp.concatenate([cum, fcum], axis=0)
    all_dt = jnp.concatenate([dt, fdt], axis=0)
    weight = expand(all_dt * jnp.exp(-all_cum), shard)
    grown = expand(jnp.concatenate([jnp.exp(all_cum), jnp.broadcast_to(skip_ref[...], (8, HEADS))], axis=0), shard)
    decay, skip = grown[:EXT], grown[EXT : EXT + 1]
    fx = jnp.concatenate([fx_ref[0].astype(F32), fx_ref[1].astype(F32)], axis=0)
    fz = jnp.concatenate([fz_ref[0].astype(F32), fz_ref[1].astype(F32)], axis=0)
    x = x_ref[...].astype(F32)
    hi, lo = split2(x * weight[:ROWS])
    b, c = b_ref[...], c_ref[...]
    fb = jnp.concatenate([fb_ref[0].astype(F32), fb_ref[1].astype(F32)], axis=0).astype(BF16)
    fc = jnp.concatenate([fc_ref[0].astype(F32), fc_ref[1].astype(F32)], axis=0).astype(BF16)
    lower = iota((ROWS, ROWS), 0) >= iota((ROWS, ROWS), 1)
    pairing = jnp.concatenate([jnp.where(lower, mm_nt(c, b), 0.0), mm_nt(fc, b)], axis=0)
    p_hi, p_lo = split2(pairing)
    inside = mm(p_hi, hi) + mm(p_hi, lo) + mm(p_lo, hi)
    own = jnp.where(chain, mm_nt(fc, fb), 0.0)
    fscaled = fx * weight[ROWS:]
    tail = inside[ROWS:]
    for r in range(FORKS):
        tail = tail + own[:, r : r + 1] * fscaled[r : r + 1]
    z = z_ref[...].astype(F32)
    gate = z / (1.0 + jnp.exp(-z))
    fgate = fz / (1.0 + jnp.exp(-fz))
    g_ref[:ROWS] = (decay[:ROWS] * inside[:ROWS] + skip * x) * gate
    g_ref[ROWS:] = (decay[ROWS:] * tail + skip * fx) * fgate
    f_ref[:ROWS] = decay[:ROWS] * gate
    f_ref[ROWS:] = decay[ROWS:] * fgate


def enter_kernel(first, pos, *refs):
    if first:
        coded_ref, c_ref, fc_ref, f_ref, g_ref, out_ref, sum_ref = refs
    else:
        coded_ref, c_ref, fc_ref, f_ref, before_ref, g_ref, out_ref, sum_ref = refs
    v = coded_ref[...].astype(jnp.int32).astype(F32)
    scale = jnp.exp2(v[N : N + 1] * (1.0 / 256.0)) * (1.0 / TOP_CODE)
    high = jnp.floor(v[:N] * (1.0 / 256.0) + 0.5)
    low = v[:N] - high * 256.0
    stacked = jnp.concatenate([high, low], axis=0).astype(BF16)
    c = jnp.concatenate([c_ref[...].astype(F32), fc_ref[0].astype(F32), fc_ref[1].astype(F32)], axis=0)
    c = jnp.concatenate([c * 256.0, c], axis=1).astype(BF16)
    gated = g_ref[...] + f_ref[...] * (mm(c, stacked) * scale)
    out_ref[...] = gated
    hi, lo = split2(gated * gated)
    ones = jnp.ones((8, SHARD), BF16)
    sums = mm_nt(ones, hi) + mm_nt(ones, lo)
    sum_ref[...] = sums if first else before_ref[...] + sums


def norm_kernel(pos, count_ref, g_ref, s0, s1, s2, s3, gain_ref, out_ref, fork_ref):
    total = (s0[...] + s1[...]) + (s2[...] + s3[...])
    inverse = lax.rsqrt(total[:1] * (1.0 / (4 * WIDTH)) + EPSILON)
    eye = iota((EXT, EXT), 0) == iota((EXT, EXT), 1)
    column = jnp.sum(jnp.where(eye, jnp.broadcast_to(inverse, (EXT, EXT)), 0.0), axis=1, keepdims=True)
    value = g_ref[...] * column * gain_ref[...]
    out_ref[...] = value[:ROWS].astype(BF16)
    for slot in range(2):
        live = (slot < count_ref[0]).astype(F32)
        fork_ref[slot] = (value[ROWS + 4 * slot : ROWS + 4 * slot + 4] * live).astype(BF16)


def query_rows(ref, g):
    pair = jnp.concatenate([ref[0].astype(F32), ref[1].astype(F32)], axis=0)
    base = g * 8 * HEAD_DIMENSION
    return jnp.concatenate([pair[:, base + q * HEAD_DIMENSION : base + (q + 1) * HEAD_DIMENSION] for q in range(8)], axis=0)


SCALE = HEAD_DIMENSION ** (-0.5)


def attention_kernel(pos, *refs):
    keys, q0, q4, q2, q1 = refs[:8], refs[8], refs[9], refs[10], refs[11]
    odd_ref, even_ref, scores = refs[12], refs[13], refs[14]
    sources = {0: q0, 4: q4, 2: q2.at[0], 6: q2.at[1], 1: q1.at[0], 5: q1.at[1], 3: q1.at[2], 7: q1.at[3]}
    eye = iota((HEAD_DIMENSION, HEAD_DIMENSION), 0) == iota((HEAD_DIMENSION, HEAD_DIMENSION), 1)
    peaks, weights, values = [], [], []
    for g in range(2):
        q = jnp.concatenate([query_rows(sources[m], g) for m in range(8)], axis=0).astype(BF16)
        lanes = slice(g * HEAD_DIMENSION, (g + 1) * HEAD_DIMENSION)
        best = None
        for i in range(8):
            s = mm_nt(q, keys[i][:ROWS, lanes])
            core = pos[1] if i < 4 else 1 - pos[1]
            seen = core * 4 + lax.rem(pos[0] + 4 - i % 4, 4) <= pos[1] * 4 + pos[0]
            s = jnp.concatenate([jnp.where(seen, s[:64], FLOOR_SCORE), s[64:]], axis=0)
            scores[:, i * ROWS : (i + 1) * ROWS] = s
            best = s if best is None else jnp.maximum(best, s)
        peak = jnp.max(best, axis=1, keepdims=True)
        total = acc = None
        for i in range(8):
            p = jnp.exp((scores[:, i * ROWS : (i + 1) * ROWS] - peak) * SCALE)
            hi, lo = split2(p)
            v = keys[i][ROWS:, lanes]
            part = mm(hi, v) + mm(lo, v)
            acc = part if acc is None else acc + part
            total = p if total is None else total + p
        peaks.append(peak)
        weights.append(jnp.sum(total, axis=1, keepdims=True))
        values.append(acc)
    for m in range(8):
        ref = even_ref if m % 2 == 0 else odd_ref
        other = lax.bitwise_xor(pos[2], m)
        good = (other >= pos[2]).astype(F32)
        rows = slice(m * 64, (m + 1) * 64)
        peak = jnp.concatenate([peaks[0][rows], peaks[1][rows]], axis=0)
        weight = jnp.concatenate([weights[0][rows], weights[1][rows]], axis=0)
        value = jnp.concatenate([values[0][rows], values[1][rows]], axis=0)
        peak_row = jnp.sum(jnp.where(eye, peak, 0.0), axis=0, keepdims=True)
        weight_row = jnp.sum(jnp.where(eye, weight, 0.0), axis=0, keepdims=True)
        peak_row = jnp.where(good > 0.0, peak_row, FLOOR_SCORE)
        row = iota((8, HEAD_DIMENSION), 0)
        ref[m // 2, :N] = value * good
        ref[m // 2, N:] = jnp.where(row == 0, peak_row, weight_row * good)


def merged(a, b, eye):
    peak = jnp.maximum(a[N : N + 1], b[N : N + 1])
    wa, wb = jnp.exp((a[N : N + 1] - peak) * SCALE), jnp.exp((b[N : N + 1] - peak) * SCALE)
    ca = jnp.sum(jnp.where(eye, wa, 0.0), axis=1, keepdims=True)
    cb = jnp.sum(jnp.where(eye, wb, 0.0), axis=1, keepdims=True)
    return a[:N] * ca + b[:N] * cb, peak, a[N + 1 : N + 2] * wa + b[N + 1 : N + 2] * wb


def merge_kernel(count, pos, keep_ref, got_ref, *outs):
    eye = iota((N, N), 0) == iota((N, N), 1)
    row = iota((8, N), 0)
    for m in range(count):
        value, peak, weight = merged(keep_ref[m], got_ref[m], eye)
        ref = outs[m % 2]
        ref[m // 2, :N] = value
        ref[m // 2, N:] = jnp.where(row == 0, peak, weight)


def finish_kernel(pos, count_ref, keep_ref, got_ref, q_ref, fk_ref, fv_ref, out_ref):
    eye = iota((N, N), 0) == iota((N, N), 1)
    value, peak, weight = merged(keep_ref[0], got_ref[0], eye)
    peak_col = jnp.sum(jnp.where(eye, peak, 0.0), axis=1, keepdims=True)
    weight_col = jnp.sum(jnp.where(eye, weight, 0.0), axis=1, keepdims=True)
    fk = jnp.concatenate([fk_ref[0].astype(F32), fk_ref[1].astype(F32)], axis=0).astype(BF16)
    fv = jnp.concatenate([fv_ref[0].astype(F32), fv_ref[1].astype(F32)], axis=0).astype(BF16)
    row, key = lax.rem(iota((64, FORKS), 0), FORKS), iota((64, FORKS), 1)
    seen = (row >= key) & (row // 4 == key // 4)
    pieces = []
    for g in range(2):
        lanes = slice(g * HEAD_DIMENSION, (g + 1) * HEAD_DIMENSION)
        rows = slice(g * 64, (g + 1) * 64)
        s = jnp.where(seen, mm_nt(query_rows(q_ref, g).astype(BF16), fk[:, lanes]), FLOOR_SCORE)
        top = jnp.maximum(peak_col[rows], jnp.max(s, axis=1, keepdims=True))
        p = jnp.where(seen, jnp.exp((s - top) * SCALE), 0.0)
        shrink = jnp.exp((peak_col[rows] - top) * SCALE)
        hi, lo = split2(p)
        v = fv[:, lanes]
        total = weight_col[rows] * shrink + jnp.sum(p, axis=1, keepdims=True)
        result = (value[rows] * shrink + mm(hi, v) + mm(lo, v)) / total
        pieces += [result[q * 8 : (q + 1) * 8] for q in range(8)]
    joined = jnp.concatenate(pieces, axis=1)
    for slot in range(2):
        live = (slot < count_ref[0]).astype(F32)
        out_ref[slot] = (joined[4 * slot : 4 * slot + 4] * live).astype(BF16)


def rotate(value, axis, count, k):
    return lax.ppermute(value, axis, [(i, (i + k) % count) for i in range(count)])


def exchange(value, axis, count, k):
    return lax.ppermute(value, axis, [(i, i ^ k) for i in range(count)])


def on_device(
    prompt_x,
    prompt_z,
    prompt_b,
    prompt_c,
    prompt_dt,
    rate_log,
    skip_scale,
    norm_gain,
    prefix_key_rows,
    prefix_value_rows,
    fork_counts,
    fork_x,
    fork_z,
    fork_b,
    fork_c,
    fork_dt,
    fork_queries,
    fork_keys,
    branch_value_rows,
):
    which = jnp.arange(3)
    pos = jnp.where(
        which == 0, lax.axis_index("rep"), jnp.where(which == 1, lax.axis_index("ctx_1"), lax.axis_index("ctx_0"))
    ).astype(jnp.int32)
    rate = rate_log.reshape(1, HEADS)
    skip = skip_scale.reshape(1, HEADS)
    gain = norm_gain.reshape(1, WIDTH)
    smem = pl.BlockSpec(memory_space=pltpu.SMEM)

    kv = jnp.concatenate([prefix_key_rows, prefix_value_rows], axis=0)
    kv_row = [kv] + [rotate(kv, "rep", 4, k) for k in (1, 2, 3)]

    pieces = [None] * 4
    for k in (2, 1, 3, 0):
        piece = call(
            functools.partial(state_kernel, k),
            pos,
            (prompt_dt, rate, prompt_x, prompt_b),
            [
                whole((ROWS, HEADS)),
                whole((1, HEADS)),
                pl.BlockSpec((ROWS, SHARD), lambda i, pos, k=k: (0, lax.rem(pos[0] + k, 4))),
                pl.BlockSpec((ROWS, N), lambda i, pos, k=k: (0, lax.rem(pos[0] + k, 4) // 2)),
            ],
            struct((META, SHARD), jnp.int16),
            whole((META, SHARD)),
            name=f"state{k}",
        )
        pieces[k] = piece if k == 0 else rotate(piece, "rep", 4, k)

    q4 = exchange(fork_queries, "ctx_0", 8, 4)
    two = jnp.stack([fork_queries, q4])
    q2 = exchange(two, "ctx_0", 8, 2)
    four = jnp.concatenate([two, q2])
    q1 = exchange(four, "ctx_0", 8, 1)
    kv_all = kv_row + [exchange(a, "ctx_1", 2, 1) for a in kv_row]

    token_block = pl.BlockSpec((ROWS, SHARD), lambda i, pos: (0, i))
    fork_block = pl.BlockSpec((2, 4, SHARD), lambda i, pos: (0, 0, i))
    group_block = pl.BlockSpec((ROWS, N), lambda i, pos: (0, i // 2))
    fork_group = pl.BlockSpec((2, 4, N), lambda i, pos: (0, 0, i // 2))
    ext_block = pl.BlockSpec((EXT, SHARD), lambda i, pos: (0, i))
    gated, factor = call(
        local_kernel,
        pos,
        (prompt_dt, rate, skip, prompt_x, prompt_z, prompt_b, prompt_c, fork_dt, fork_x, fork_z, fork_b, fork_c),
        [
            whole((ROWS, HEADS)),
            whole((1, HEADS)),
            whole((1, HEADS)),
            token_block,
            token_block,
            group_block,
            group_block,
            whole((2, 4, HEADS)),
            fork_block,
            fork_block,
            fork_group,
            fork_group,
        ],
        (struct((EXT, WIDTH)), struct((EXT, WIDTH))),
        (ext_block, ext_block),
        grid=(4,),
        flops=4 * 10**9,
        name="local",
    )

    coded_shape = (META, SHARD)
    row = call(
        row_kernel,
        pos,
        pieces,
        [whole(coded_shape)] * 4,
        struct(coded_shape),
        whole(coded_shape),
        scratch=[pltpu.VMEM((4, *coded_shape), jnp.int16)],
        name="row",
    )
    row_other = exchange(row, "ctx_1", 2, 1)
    half_shape = (META, HALF)
    half_of = pl.BlockSpec(half_shape, lambda i, pos: (0, pos[1]))
    total, coded = call(
        plane_kernel,
        pos,
        (row, row_other),
        [half_of, half_of],
        (struct(half_shape), struct(half_shape, jnp.int16)),
        (whole(half_shape), whole(half_shape)),
        name="plane",
    )
    before = None
    for bit in range(3):
        got = exchange(coded, "ctx_0", 8, 1 << bit)
        last = bit == 2
        operands = (total, got) if bit == 0 else (total, before, got)
        outs = [struct(half_shape)] if last else [struct(half_shape), struct(half_shape), struct(half_shape, jnp.int16)]
        result = call(
            functools.partial(scan_kernel, bit, last),
            pos,
            operands,
            [whole(half_shape)] * len(operands),
            outs,
            [whole(half_shape)] * len(outs),
            name=f"scan{bit}",
        )
        before = result[0]
        if not last:
            _, total, coded = result
    before_other = exchange(before, "ctx_1", 2, 1)
    entering = call(
        return_kernel,
        pos,
        (*pieces, before, before_other, row_other),
        [whole(coded_shape)] * 4 + [whole(half_shape)] * 2 + [whole(coded_shape)],
        [struct(coded_shape, jnp.int16)] * 4,
        [whole(coded_shape)] * 4,
        scratch=[pltpu.VMEM((4, *coded_shape), jnp.int16), pltpu.VMEM((4, N, SHARD), F32)],
        name="prefixes",
    )
    entering = [entering[0]] + [rotate(entering[k], "rep", 4, k) for k in (1, 2, 3)]

    part_shape = (4, META, N)
    odd, even = call(
        attention_kernel,
        pos,
        (*kv_all, fork_queries, q4, q2, q1),
        [whole((2 * ROWS, 2 * HEAD_DIMENSION))] * 8
        + [whole((2, 4, 2048)), whole((2, 4, 2048)), whole((2, 2, 4, 2048)), whole((4, 2, 4, 2048))],
        (struct(part_shape), struct(part_shape)),
        (whole(part_shape), whole(part_shape)),
        scratch=[pltpu.VMEM((512, 8 * ROWS), F32)],
        flops=4 * 10**9,
        name="attention",
    )
    send, keep = odd, even
    for bit, count in ((0, 4), (1, 2)):
        got = exchange(send, "ctx_0", 8, 1 << bit)
        shape, part = (count, META, N), (count // 2, META, N)
        keep, send = call(
            functools.partial(merge_kernel, count),
            pos,
            (keep, got),
            [whole(shape)] * 2,
            (struct(part), struct(part)),
            (whole(part), whole(part)),
            name=f"merge{bit}",
        )
    got = exchange(send, "ctx_0", 8, 4)
    fork_attn = call(
        finish_kernel,
        pos,
        (fork_counts, keep, got, fork_queries, fork_keys, branch_value_rows),
        [smem, whole((1, META, N)), whole((1, META, N)), whole((2, 4, 2048)), whole((2, 4, 256)), whole((2, 4, 256))],
        struct((2, 4, 2048), BF16),
        whole((2, 4, 2048)),
        name="finish",
    )

    sums = None
    for k in range(4):
        source = lambda i, pos, k=k: (0, lax.rem(pos[0] + 4 - k, 4))
        group = lambda i, pos, k=k: (0, lax.rem(pos[0] + 4 - k, 4) // 2)
        fork_of = lambda i, pos, k=k: (0, 0, lax.rem(pos[0] + 4 - k, 4) // 2)
        operands = [entering[k], prompt_c, fork_c, factor] + ([] if k == 0 else [sums]) + [gated]
        specs = [
            whole(coded_shape),
            pl.BlockSpec((ROWS, N), group),
            pl.BlockSpec((2, 4, N), fork_of),
            pl.BlockSpec((EXT, SHARD), source),
        ]
        specs += ([] if k == 0 else [whole((8, EXT))]) + [pl.BlockSpec((EXT, SHARD), source)]
        gated, sums = call(
            functools.partial(enter_kernel, k == 0),
            pos,
            operands,
            specs,
            (struct((EXT, WIDTH)), struct((8, EXT))),
            (pl.BlockSpec((EXT, SHARD), source), whole((8, EXT))),
            alias={len(operands): 0},
            flops=10**9,
            name=f"enter{k}",
        )
    others = [rotate(sums, "tp", 4, k) for k in (1, 2, 3)]
    prompt_out, fork_mamba = call(
        norm_kernel,
        pos,
        (fork_counts, gated, sums, *others, gain),
        [smem, ext_block] + [whole((8, EXT))] * 4 + [pl.BlockSpec((1, SHARD), lambda i, pos: (0, i))],
        (struct((ROWS, WIDTH), BF16), struct((2, 4, WIDTH), BF16)),
        (token_block, fork_block),
        grid=(4,),
        name="norm",
    )
    return prompt_out, fork_mamba, fork_attn


def solution(mesh):
    split = Mesh(
        mesh.devices.reshape(8, 2, mesh.shape["rep"], mesh.shape["tp"]),
        ("ctx_0", "ctx_1", "rep", "tp"),
    )
    tokens, forks = P(CTX_REP, "tp"), P(CTX_REP, None, "tp")
    return jax.shard_map(
        on_device,
        mesh=split,
        in_specs=(tokens,) * 5 + (P("tp"),) * 3 + (tokens,) * 2 + (P(CTX_REP),) + (forks,) * 8,
        out_specs=(tokens, forks, forks),
        check_vma=False,
    )
```
